32 devices in a mesh: crop: 2 (over x), seq: 2 (over y), res: 8 (over z, core).
Axes of the slice: x: 2, y: 2, z: 4, core: 2. Of those that a mesh axis runs over, the one named last changes fastest.
Arguments:
- aligned_chain_embedding: bfloat16 [128, 32, 256], P(('crop', 'seq'), 'res'), parts along dimension 0, may hold values from -6 to 6
- alignment_mask: int32 [128, 32], P(('crop', 'seq'), 'res'), parts along dimension 0, may hold values from 0 to 1, as said below
- resolved_residue_mask: int32 [64], P('crop'), parts along dimension 0, may hold values 0 or 1
- pairwise_state: bfloat16 [64, 32, 128], P(('crop', 'seq'), 'res'), parts along dimension 0, may hold values from -8 to 8
- combined_projection_matrix: bfloat16 [256, 1024], replicated, may hold values from -0.375 to 0.375
- pair_bias_weight: bfloat16 [128, 8], replicated, may hold values from -8 to 8
- final_projection_matrix: bfloat16 [256, 256], replicated, may hold values from -0.375 to 0.375
- left_right_projection_matrix: bfloat16 [256, 64], replicated, may hold values from -1.5 to 1.5
- outer_mean_weight: bfloat16 [1024, 128], replicated, may hold values from -0.1875 to 0.1875
Outputs:
- alignment_output: bfloat16 [128, 32, 256], P(('crop', 'seq'), 'res'), parts along dimension 0
- pairwise_output: bfloat16 [64, 32, 128], P(('crop', 'seq'), 'res'), parts along dimension 0
The draws below stay inside these ranges and needn't reach their ends.
There are 2 independent parts, one for each index of `crop`. The reference program is written for one: setup_inputs(seed, part) draws one part's arguments, and reference() takes and returns one part's arrays. A program takes and returns all parts, laid end to end along the dimension named above; an argument that names none is the same for every part. Nothing has to cross between parts.
Inputs may be any that keep to these rules, and one draw needn't show every extreme that they name: `alignment_mask`: sequence 0 has no gaps.
All inputs are finite; a program needn't handle non-finite values.
Results may differ from the reference program's by a relative error of at most 0.013.
The reference program's roundings to bfloat16 on the way count: a program that leaves them out, or rounds other values in their place, can miss the bound.
Values may be sent and summed in bfloat16 or wider, within the bound.
A program may use at most 64 MiB of HBM per device.

```python
import math
import jax
import jax.numpy as jnp
from jax import lax

ROW_FEATURES = 256
CZ = 128
HEAD_NUMBER = 8
PER_HEAD_DIM = 32
PROJ_FEATURES = 32
ALIGNED_CHAINS = 64
WINDOW_AMINOS = 32


def draw_alignment_mask(key, part):
    permutation_indices = jnp.arange(ALIGNED_CHAINS, dtype=jnp.int32)[:, None]
    uniform_bound = 900 - 600 * permutation_indices // max(ALIGNED_CHAINS - 1, 1)
    random_token = jax.random.randint(key, (ALIGNED_CHAINS, WINDOW_AMINOS), 0, 1000, dtype=jnp.int32)
    keep = jnp.logical_or(random_token < uniform_bound, permutation_indices == 0)
    return keep.astype(jnp.int32)


def draw_pairwise_state(key, part):
    noise_key = jax.random.fold_in(key, 0)
    noise = jax.random.normal(noise_key, (WINDOW_AMINOS, WINDOW_AMINOS, CZ), jnp.float32)
    return jnp.clip(noise, -8.0, 8.0).astype(jnp.bfloat16)


def draw_pair_bias_weight(key, part):
    base_key = jax.random.fold_in(key, 0)
    weights = jax.random.normal(base_key, (CZ, HEAD_NUMBER), jnp.float32) / math.sqrt(CZ)
    return jnp.clip(weights, -8.0, 8.0).astype(jnp.bfloat16)


def set_ends(values, own_key, low, high):
    longest = values.shape.index(max(values.shape))
    spots = []
    for shift in (0, 1):
        where = [jax.random.randint(jax.random.fold_in(own_key, axis), (), 0, length) for axis, length in enumerate(values.shape)]
        where[longest] = (where[longest] + shift) % values.shape[longest]
        spots.append(tuple(where))
    return values.at[spots[0]].set(low).at[spots[1]].set(high)


def block_scale(stream_key, extent, shards, least, largest):
    factor_of, own = 1.0, jax.random.fold_in(stream_key, 6)
    for position, blocks in shards:
        heights = jnp.exp(jax.random.uniform(jax.random.fold_in(own, position), (blocks,), jnp.float32, least / len(shards), largest / len(shards)))
        factor_of = factor_of * jnp.repeat(heights, extent[position] // blocks).reshape([-1 if axis == position else 1 for axis in range(len(extent))])
    return factor_of


def scatter_about(rng, shape, spread, bound, cuts=(), kind=jnp.bfloat16):
    level = block_scale(rng, shape, cuts, -0.22, 0.18) if cuts else 1.0
    values = jax.random.normal(rng, shape, jnp.float32) * spread * level
    return jnp.minimum(jnp.maximum(values, -bound), bound).astype(kind)


def setup_inputs(seed: int = 0, part: int = 0) -> dict:
    key_of = jax.random.split(jax.random.key(seed), 10)
    part_keys = jax.random.split(jax.random.fold_in(key_of[9], part), 10)
    return {
        "aligned_chain_embedding": scatter_about(part_keys[0], (ALIGNED_CHAINS, WINDOW_AMINOS, ROW_FEATURES), 1.0, 6.0, ((0, 2), (1, 8))),
        "alignment_mask": draw_alignment_mask(jax.random.fold_in(jax.random.fold_in(key_of[9], part), 71), part),
        "resolved_residue_mask": set_ends((jax.random.randint(part_keys[2], (WINDOW_AMINOS,), 0, 5) < 4).astype(jnp.int32), jax.random.fold_in(part_keys[2], 1), 0, 1),
        "pairwise_state": draw_pairwise_state(jax.random.fold_in(jax.random.fold_in(key_of[9], part), 71), part),
        "combined_projection_matrix": scatter_about(key_of[4], (ROW_FEATURES, 4 * ROW_FEATURES), ROW_FEATURES ** -0.5, 0.375),
        "pair_bias_weight": draw_pair_bias_weight(jax.random.fold_in(key_of[9], 71), part),
        "final_projection_matrix": scatter_about(key_of[6], (ROW_FEATURES, ROW_FEATURES), ROW_FEATURES ** -0.5, 0.375),
        "left_right_projection_matrix": scatter_about(key_of[7], (ROW_FEATURES, 2 * PROJ_FEATURES), (ROW_FEATURES // 16) ** -0.5, 1.5),
        "outer_mean_weight": scatter_about(key_of[8], (PROJ_FEATURES * PROJ_FEATURES, CZ), (PROJ_FEATURES * PROJ_FEATURES) ** -0.5, 0.1875),
    }


epsilon = 1e-05

def layer_normalize(values):
    values = values.astype(jnp.float32)
    average = lax.optimization_barrier(jnp.mean(values, axis=-1, keepdims=True))
    centered = values - average
    variance = lax.optimization_barrier(jnp.mean(centered * centered, axis=-1, keepdims=True))
    return centered * lax.rsqrt(variance + epsilon)

def reference(aligned_chain_embedding, alignment_mask, resolved_residue_mask, pairwise_state, combined_projection_matrix, pair_bias_weight, final_projection_matrix, left_right_projection_matrix, outer_mean_weight):
    standardized_rows = layer_normalize(aligned_chain_embedding).astype(jnp.bfloat16)
    linear_mapped = jnp.dot(standardized_rows.reshape(ALIGNED_CHAINS * WINDOW_AMINOS, ROW_FEATURES), combined_projection_matrix, preferred_element_type=jnp.float32)
    linear_mapped = linear_mapped.reshape(ALIGNED_CHAINS, WINDOW_AMINOS, 4, HEAD_NUMBER, PER_HEAD_DIM)
    queries = (linear_mapped[:, :, 0] * PER_HEAD_DIM ** (-0.5)).astype(jnp.bfloat16)
    key_rows = linear_mapped[:, :, 1].astype(jnp.bfloat16)
    value_rows = linear_mapped[:, :, 2].astype(jnp.bfloat16)
    sigmoid_factor = jax.nn.sigmoid(linear_mapped[:, :, 3])
    pair_normed = layer_normalize(pairwise_state).astype(jnp.bfloat16)
    head_bias = jnp.dot(pair_normed.reshape(WINDOW_AMINOS * WINDOW_AMINOS, CZ), pair_bias_weight, preferred_element_type=jnp.float32)
    head_bias = jnp.transpose(head_bias.astype(jnp.bfloat16).reshape(WINDOW_AMINOS, WINDOW_AMINOS, HEAD_NUMBER), (2, 0, 1)).astype(jnp.float32)
    key_validity_mask = (alignment_mask.astype(jnp.float32) - 1.0) * 1000000000.0

    def attend(inputs):
        query_one, key_one, value_one, mask_one = inputs
        scores = jnp.einsum('ihd,jhd->hij', query_one.astype(jnp.float32), key_one.astype(jnp.float32), precision=lax.Precision.HIGHEST)
        scores = scores + head_bias + mask_one[None, None, :]
        row_max = lax.optimization_barrier(jnp.max(scores, axis=-1, keepdims=True))
        exponent = jnp.exp(scores - row_max)
        weights = (exponent / lax.optimization_barrier(jnp.sum(exponent, axis=-1, keepdims=True))).astype(jnp.bfloat16)
        result = jnp.einsum('hij,jhd->ihd', weights.astype(jnp.float32), value_one.astype(jnp.float32), precision=lax.Precision.HIGHEST)
        return result.astype(jnp.bfloat16)
    softmax_mixed = lax.map(attend, (queries, key_rows, value_rows, key_validity_mask))
    sigmoid_scaled = (sigmoid_factor * softmax_mixed.astype(jnp.float32)).astype(jnp.bfloat16).reshape(ALIGNED_CHAINS * WINDOW_AMINOS, ROW_FEATURES)
    embedding_increment = jnp.dot(sigmoid_scaled, final_projection_matrix, preferred_element_type=jnp.float32).reshape(ALIGNED_CHAINS, WINDOW_AMINOS, ROW_FEATURES)
    alignment_output = (aligned_chain_embedding.astype(jnp.float32) + embedding_increment).astype(jnp.bfloat16)
    standardized_product = layer_normalize(alignment_output).astype(jnp.bfloat16)
    left_right_vectors = jnp.dot(standardized_product.reshape(ALIGNED_CHAINS * WINDOW_AMINOS, ROW_FEATURES), left_right_projection_matrix, preferred_element_type=jnp.float32).reshape(ALIGNED_CHAINS, WINDOW_AMINOS, 2, PROJ_FEATURES)
    entry_present = alignment_mask.astype(jnp.float32)[:, :, None]
    left_side = (left_right_vectors[:, :, 0] * entry_present).astype(jnp.bfloat16)
    right_side = (left_right_vectors[:, :, 1] * entry_present).astype(jnp.bfloat16)
    presence_mask_flags = alignment_mask.astype(jnp.bfloat16)
    counts = jnp.dot(presence_mask_flags.T, presence_mask_flags, preferred_element_type=jnp.float32)
    project = outer_mean_weight.astype(jnp.float32)
    block_rows = math.gcd(32, WINDOW_AMINOS)

    def outer_block(start):
        left_piece = lax.dynamic_slice_in_dim(left_side, start, block_rows, 1)
        product = jnp.einsum('sic,sje->ijce', left_piece.astype(jnp.float32), right_side.astype(jnp.float32), precision=lax.Precision.HIGHEST)
        flattened = product.reshape(block_rows * WINDOW_AMINOS, PROJ_FEATURES * PROJ_FEATURES)
        return jnp.dot(flattened, project, precision=lax.Precision.HIGHEST).reshape(block_rows, WINDOW_AMINOS, CZ)
    starts = jnp.arange(WINDOW_AMINOS // block_rows, dtype=jnp.int32) * block_rows
    outer = lax.map(outer_block, starts).reshape(WINDOW_AMINOS, WINDOW_AMINOS, CZ)
    pair_mask = (resolved_residue_mask[:, None] * resolved_residue_mask[None, :]).astype(jnp.float32)
    pairwise_output = (pairwise_state.astype(jnp.float32) + pair_mask[:, :, None] * (outer / counts[:, :, None])).astype(jnp.bfloat16)
    return (alignment_output, pairwise_output)
```

```python
import functools
import math

import jax
import jax.numpy as jnp
from jax import lax
from jax.experimental import pallas as pl
from jax.experimental.pallas import tpu as pltpu
from jax.sharding import PartitionSpec as P

ROW_FEATURES = 256
CZ = 128
HEAD_NUMBER = 8
PER_HEAD_DIM = 32
PROJ_FEATURES = 32


epsilon = 1e-05


def layer_normalize(values):
    values = values.astype(jnp.float32)
    average = jnp.mean(values, axis=-1, keepdims=True)
    centered = values - average
    variance = jnp.mean(centered * centered, axis=-1, keepdims=True)
    return centered * lax.rsqrt(variance + epsilon)


def outer_rows(left_side, right_side, project):
    row_total = left_side.shape[1]
    col_total = right_side.shape[1]
    block_rows = math.gcd(row_total, max(1, 2048 // col_total))

    def outer_block(start):
        product = jnp.einsum(
            "sic,sje->ijce", left_side, right_side, preferred_element_type=jnp.float32
        )
        flattened = product.reshape(block_rows * col_total, PROJ_FEATURES * PROJ_FEATURES)
        return jnp.dot(flattened, project, precision=lax.Precision.HIGHEST).reshape(
            block_rows, col_total, CZ
        )

    starts = jnp.arange(row_total // block_rows, dtype=jnp.int32) * block_rows
    return lax.map(outer_block, starts).reshape(row_total, col_total, CZ)


def per_device(
    aligned_chain_embedding,
    alignment_mask,
    resolved_residue_mask,
    pairwise_state,
    combined_projection_matrix,
    pair_bias_weight,
    final_projection_matrix,
    left_right_projection_matrix,
    outer_mean_weight,
):
    chain_count = aligned_chain_embedding.shape[0]
    amino_count = aligned_chain_embedding.shape[1]
    res_ranks = lax.axis_size("res")
    seq_groups = lax.axis_size("seq")
    full_length = amino_count * res_ranks
    row_count = full_length // seq_groups
    item_count = HEAD_NUMBER * chain_count // res_ranks
    per_head = min(item_count, chain_count)
    head_count = item_count // per_head
    my_rank = lax.axis_index("res")
    my_group = lax.axis_index("seq")
    standardized_rows = layer_normalize(aligned_chain_embedding).astype(jnp.bfloat16)
    linear_mapped = jnp.dot(
        standardized_rows.reshape(chain_count * amino_count, ROW_FEATURES),
        combined_projection_matrix,
        preferred_element_type=jnp.float32,
    )
    linear_mapped = linear_mapped.reshape(chain_count, amino_count, 4, HEAD_NUMBER, PER_HEAD_DIM)
    queries = (linear_mapped[:, :, 0] * PER_HEAD_DIM ** (-0.5)).astype(jnp.bfloat16)
    key_rows = linear_mapped[:, :, 1].astype(jnp.bfloat16)
    value_rows = linear_mapped[:, :, 2].astype(jnp.bfloat16)
    sigmoid_factor = jax.nn.sigmoid(linear_mapped[:, :, 3])
    stacked = jnp.stack([queries, key_rows, value_rows], axis=2)
    stacked = jnp.transpose(stacked, (3, 0, 1, 2, 4)).reshape(
        HEAD_NUMBER * chain_count, amino_count, 3 * PER_HEAD_DIM
    )
    presence_mask_flags = alignment_mask.astype(jnp.bfloat16)
    key_flags = jnp.broadcast_to(
        presence_mask_flags[None], (HEAD_NUMBER, chain_count, amino_count)
    ).reshape(HEAD_NUMBER * chain_count, amino_count)
    arrived, arrived_flags = (
        lax.all_to_all(stacked, "res", split_axis=0, concat_axis=1, tiled=True),
        lax.all_to_all(key_flags, "res", split_axis=0, concat_axis=1, tiled=True),
    )
    pair_normed = layer_normalize(pairwise_state).astype(jnp.bfloat16)
    local_bias = jnp.dot(
        pair_normed.reshape(row_count * amino_count, CZ),
        pair_bias_weight,
        preferred_element_type=jnp.float32,
    )
    local_bias = jnp.transpose(
        local_bias.astype(jnp.bfloat16).reshape(row_count, amino_count, HEAD_NUMBER), (2, 0, 1)
    )
    bias_cols = lax.all_gather(local_bias, "res", axis=2, tiled=True)
    whole_bias = lax.all_gather(bias_cols, "seq", axis=1, tiled=True)
    first_head = my_rank * item_count // chain_count
    head_bias = lax.dynamic_slice_in_dim(whole_bias, first_head, head_count, 0)
    grouped = arrived.reshape(head_count, per_head, full_length, 3, PER_HEAD_DIM)
    key_validity_mask = (
        arrived_flags.reshape(head_count, per_head, full_length).astype(jnp.float32) - 1.0
    ) * 1000000000.0
    scores = jnp.einsum(
        "gpid,gpjd->gpij",
        grouped[:, :, :, 0],
        grouped[:, :, :, 1],
        preferred_element_type=jnp.float32,
    )
    scores = scores + head_bias.astype(jnp.float32)[:, None] + key_validity_mask[:, :, None, :]
    row_max = jnp.max(scores, axis=-1, keepdims=True)
    exponent = jnp.exp(scores - row_max)
    weights = (exponent / jnp.sum(exponent, axis=-1, keepdims=True)).astype(jnp.bfloat16)
    softmax_mixed = jnp.einsum(
        "gpij,gpjd->gpid", weights, grouped[:, :, :, 2], preferred_element_type=jnp.float32
    )
    softmax_mixed = softmax_mixed.astype(jnp.bfloat16).reshape(
        item_count, full_length, PER_HEAD_DIM
    )
    returned = lax.all_to_all(softmax_mixed, "res", split_axis=1, concat_axis=0, tiled=True)
    returned = jnp.transpose(
        returned.reshape(HEAD_NUMBER, chain_count, amino_count, PER_HEAD_DIM), (1, 2, 0, 3)
    )
    sigmoid_scaled = (
        (sigmoid_factor * returned.astype(jnp.float32))
        .astype(jnp.bfloat16)
        .reshape(chain_count * amino_count, ROW_FEATURES)
    )
    embedding_increment = jnp.dot(
        sigmoid_scaled, final_projection_matrix, preferred_element_type=jnp.float32
    ).reshape(chain_count, amino_count, ROW_FEATURES)
    alignment_output = (aligned_chain_embedding.astype(jnp.float32) + embedding_increment).astype(
        jnp.bfloat16
    )
    standardized_product = layer_normalize(alignment_output).astype(jnp.bfloat16)
    left_right_vectors = jnp.dot(
        standardized_product.reshape(chain_count * amino_count, ROW_FEATURES),
        left_right_projection_matrix,
        preferred_element_type=jnp.float32,
    )
    left_right_vectors = left_right_vectors.reshape(chain_count, amino_count, 2, PROJ_FEATURES)
    entry_present = alignment_mask.astype(jnp.float32)[:, :, None]
    left_side = (left_right_vectors[:, :, 0] * entry_present).astype(jnp.bfloat16)
    right_side = (left_right_vectors[:, :, 1] * entry_present).astype(jnp.bfloat16)
    left_all, left_flags = (
        lax.all_gather(left_side, "res", axis=1, tiled=True),
        lax.all_gather(presence_mask_flags, "res", axis=1, tiled=True),
    )
    project = outer_mean_weight.astype(jnp.float32)
    row_start = my_group * row_count
    left_full, flag_full = (
        lax.all_to_all(left_all, "seq", split_axis=1, concat_axis=0, tiled=True),
        lax.all_to_all(left_flags, "seq", split_axis=1, concat_axis=0, tiled=True),
    )
    right_full, right_flags = (
        lax.all_gather(right_side, "seq", axis=0, tiled=True),
        lax.all_gather(presence_mask_flags, "seq", axis=0, tiled=True),
    )
    counts = jnp.dot(flag_full.T, right_flags, preferred_element_type=jnp.float32)
    outer = outer_rows(left_full, right_full, project)
    col_start = my_rank * amino_count
    row_mask = lax.dynamic_slice_in_dim(resolved_residue_mask, row_start, row_count).astype(
        jnp.float32
    )
    col_mask = lax.dynamic_slice_in_dim(resolved_residue_mask, col_start, amino_count).astype(
        jnp.float32
    )
    pair_mask = row_mask[:, None] * col_mask[None, :]
    pairwise_output = (
        pairwise_state.astype(jnp.float32) + pair_mask[:, :, None] * (outer / counts[:, :, None])
    ).astype(jnp.bfloat16)
    return (alignment_output, pairwise_output)


LANES = 128
F32 = jnp.float32
BF16 = jnp.bfloat16


def iota(shape, axis):
    return lax.broadcasted_iota(jnp.int32, shape, axis)


def dot(a, b, ca=1, cb=0):
    return lax.dot_general(a, b, (((ca,), (cb,)), ((), ())), preferred_element_type=F32)


def one_hot(cond):
    return jnp.where(cond, 1.0, 0.0).astype(BF16)


def fused_kernel(
    groups, ranks, chains, aminos,
    emb_ref, mask_ref, resolved_ref, pair_ref, proj_ref, bias_w_ref, final_ref, lr_ref, outer_ref,
    out_ref, pair_out_ref,
    emb_buf, aux_buf, left_send, left_buf, right_send, right_buf, out_send, out_buf,
    weight_buf, product_buf, lhs_buf,
    emb_s, emb_r, aux_s, aux_r, left_s, left_r, right_s, right_r, out_s, out_r,
):
    devices = groups * ranks
    per = chains // ranks
    tile = per * aminos
    rows = ranks * tile
    full = ranks * aminos
    pair_rows = full // groups
    pairs = pair_rows * aminos
    half = rows // groups
    group = lax.axis_index("seq")
    rank = lax.axis_index("res")
    me = group * ranks + rank

    def peer_of(k):
        peer = lax.rem(me + k, devices)
        return peer, {"seq": peer // ranks, "res": lax.rem(peer, ranks)}

    barrier = pltpu.get_barrier_semaphore()
    for k in range(1, devices):
        pl.semaphore_signal(
            barrier, inc=1, device_id=peer_of(k)[1], device_id_type=pl.DeviceIdType.MESH
        )

    def send(src, dst, ssem, rsem, device):
        copy = pltpu.make_async_remote_copy(
            src_ref=src, dst_ref=dst, send_sem=ssem, recv_sem=rsem,
            device_id=device, device_id_type=pl.DeviceIdType.MESH,
        )
        copy.start()
        return copy

    pair_value = pair_ref[...]
    pair_normed = layer_normalize(pair_value).astype(BF16)
    wide = jnp.concatenate([pair_normed] * groups, axis=0)
    wide = jnp.where(iota((groups * pairs, CZ), 0) // pairs == group, wide, jnp.zeros_like(wide))
    own_bias = dot(bias_w_ref[...], wide, 0, 1)
    spread = dot(mask_ref[...].astype(F32).astype(BF16), one_hot(
        iota((aminos, LANES), 1) % aminos == iota((aminos, LANES), 0)))
    flag_row = jnp.sum(
        jnp.where(iota((chains, LANES), 1) // aminos == iota((chains, LANES), 0), spread, 0.0),
        axis=0, keepdims=True)
    flags = jnp.broadcast_to(flag_row, (HEAD_NUMBER, LANES))
    aux_buf[me] = jnp.concatenate([own_bias, flags], axis=0).astype(BF16)
    emb_buf[rank] = emb_ref[rank]

    pl.semaphore_wait(barrier, devices - 1)
    pending = []
    emb_copies = []
    for k in range(1, ranks):
        peer = lax.rem(rank + k, ranks)
        emb_copies.append(send(emb_ref.at[peer], emb_buf.at[rank], emb_s.at[k], emb_r.at[k],
                               {"seq": group, "res": peer}))
    aux_copies = []
    for k in range(1, devices):
        aux_copies.append(send(aux_buf.at[me], aux_buf.at[me], aux_s.at[k], aux_r.at[k],
                               peer_of(k)[1]))

    per_c = aminos * PROJ_FEATURES
    for c in range(PROJ_FEATURES):
        piece = outer_ref[c * PROJ_FEATURES:(c + 1) * PROJ_FEATURES, :]
        for j in range(aminos):
            at = c * per_c + j * PROJ_FEATURES
            weight_buf[at:at + PROJ_FEATURES, :] = piece
    q0 = iota((pairs, pairs), 0)
    q1 = iota((pairs, pairs), 1)
    order = one_hot((q0 % pair_rows) * aminos + q0 // pair_rows == q1)
    pair_turned = dot(order, pair_value)
    lane_r = iota((pairs, full), 1)
    row_r = iota((pairs, full), 0)
    resolved = jnp.broadcast_to(resolved_ref[...].astype(F32), (pairs, full))
    pair_mask = jnp.sum(
        jnp.where(lane_r == group * pair_rows + row_r % pair_rows, resolved, 0.0),
        axis=1, keepdims=True
    ) * jnp.sum(
        jnp.where(lane_r == rank * aminos + row_r // pair_rows, resolved, 0.0),
        axis=1, keepdims=True)

    for copy in emb_copies:
        copy.wait_recv()
    embedding = emb_buf[...].reshape(rows, ROW_FEATURES)
    normed = layer_normalize(embedding).astype(BF16)
    projected = dot(normed, proj_ref[...])
    width = HEAD_NUMBER * PER_HEAD_DIM
    queries = (projected[:, :width] * PER_HEAD_DIM ** (-0.5)).astype(BF16)
    keys = projected[:, width:2 * width].astype(BF16)
    values = projected[:, 2 * width:3 * width].astype(BF16)
    gating = jax.nn.sigmoid(projected[:, 3 * width:])

    for copy in aux_copies:
        copy.wait_recv()
    aux = aux_buf[...].astype(F32)
    bias_all = aux[0:ranks, :HEAD_NUMBER]
    for g in range(1, groups):
        bias_all = bias_all + aux[g * ranks:(g + 1) * ranks, :HEAD_NUMBER]
    bias_all = bias_all.reshape(ranks * HEAD_NUMBER, LANES).astype(BF16)
    hq = (HEAD_NUMBER * rows, ranks * HEAD_NUMBER)
    pick = one_hot(
        ((iota(hq, 0) % rows) // tile) * HEAD_NUMBER + iota(hq, 0) // rows == iota(hq, 1))
    bias_q = dot(pick, bias_all)
    hl = (HEAD_NUMBER * rows, LANES)
    bias_q = jnp.where(iota(hl, 1) % aminos == iota(hl, 0) % aminos, bias_q, 0.0).astype(BF16)
    pp = iota((rows, LANES), 0)
    ll = iota((rows, LANES), 1)
    row_pick = one_hot(ll // aminos == (pp // tile) * aminos + pp % aminos)
    bias_full = dot(row_pick, bias_q, 1, 1)
    flag_all = aux[:, HEAD_NUMBER:HEAD_NUMBER + 1].reshape(devices, LANES).astype(BF16)
    near = dot(flag_all, one_hot(pp == rank * tile + ll % tile))
    near_row = jnp.sum(
        jnp.where(
            iota((devices, LANES), 0) == group * ranks + iota((devices, LANES), 1) // tile,
            near, 0.0),
        axis=0, keepdims=True)
    key_mask = (near_row - 1.0) * 1000000000.0
    present = jnp.sum(jnp.where(pp == ll, near_row, 0.0), axis=1, keepdims=True)
    same_chain = (pp // aminos) % per == (ll // aminos) % per
    heads_per = LANES // PER_HEAD_DIM
    mixed = []
    for block in range(width // LANES):
        cols = slice(block * LANES, (block + 1) * LANES)
        total = jnp.zeros((rows, LANES), F32)
        for sub in range(heads_per):
            head = block * heads_per + sub
            lanes = ll // PER_HEAD_DIM == sub
            query = jnp.where(lanes, queries[:, cols], jnp.zeros((), BF16))
            scores = dot(query, keys[:, cols], 1, 1)
            scores = scores + bias_full[:, head * rows:(head + 1) * rows] + key_mask
            scores = jnp.where(same_chain, scores, -3e38)
            exponent = jnp.exp(scores - jnp.max(scores, axis=1, keepdims=True))
            weights = (exponent / jnp.sum(exponent, axis=1, keepdims=True)).astype(BF16)
            total = jnp.where(lanes, dot(weights, values[:, cols]), total)
        mixed.append(total)
    attended = jnp.concatenate(mixed, axis=1).astype(BF16)
    gated = (gating * attended.astype(F32)).astype(BF16)
    updated = (embedding.astype(F32) + dot(gated, final_ref[...])).astype(BF16)
    normed_out = layer_normalize(updated).astype(BF16)

    folds = LANES // half
    low = PROJ_FEATURES // folds
    left_t = dot(lr_ref[:, :PROJ_FEATURES], normed_out, 0, 1) * near_row
    for g in range(groups):
        part = left_t[:, g * half:(g + 1) * half]
        left_send[g] = jnp.concatenate(
            [part[f * low:(f + 1) * low] for f in range(folds)], axis=1).astype(BF16)
    right_w = jnp.concatenate([lr_ref[:, PROJ_FEATURES:]] * aminos, axis=1)
    right = dot(normed_out, right_w) * present
    right = jnp.where(ll // PROJ_FEATURES == pp % aminos, right, 0.0).astype(BF16)
    right_send[...] = right.reshape(ranks, tile, LANES)
    out_send[...] = updated.reshape(ranks, tile, ROW_FEATURES)
    left_copies = []
    for k in range(1, devices):
        peer, device = peer_of(k)
        left_copies.append(send(left_send.at[peer // ranks], left_buf.at[me],
                                left_s.at[k], left_r.at[k], device))
        left_copies.append(send(right_send.at[lax.rem(peer, ranks)], right_buf.at[me],
                                right_s.at[k], right_r.at[k], device))
    out_copies = []
    for k in range(1, ranks):
        peer = lax.rem(rank + k, ranks)
        out_copies.append(send(out_send.at[peer], out_buf.at[rank], out_s.at[k], out_r.at[k],
                               {"seq": group, "res": peer}))
    left_buf[me] = left_send[group]
    right_buf[me] = right_send[rank]
    out_buf[rank] = out_send[rank]

    gq = (groups * pairs, devices)
    gl = (groups * pairs, LANES)
    within = iota(gl, 0) % pairs
    row_at = group * pair_rows + within % pair_rows
    group_q = iota(gq, 0) // pairs
    row_at_q = group * pair_rows + (iota(gq, 0) % pairs) % pair_rows
    row_flags = dot(one_hot(group_q * ranks + row_at_q // aminos == iota(gq, 1)), flag_all)
    col_flags = dot(one_hot(group_q * ranks + rank == iota(gq, 1)), flag_all)
    amino_l = iota(gl, 1) % aminos
    gather_s = one_hot(pp // aminos == ll)
    row_flags = dot(one_hot((amino_l == row_at % aminos) & (row_flags > 0.5)), gather_s)
    col_flags = dot(one_hot((amino_l == within // pair_rows) & (col_flags > 0.5)), gather_s)
    both = jnp.sum(row_flags * col_flags, axis=1, keepdims=True)
    counts = both[:pairs]
    for g in range(1, groups):
        counts = counts + both[g * pairs:(g + 1) * pairs]

    rep = one_hot(
        (iota((LANES, tile), 0) // aminos) % per == iota((LANES, tile), 1) // aminos)
    il = (folds * pair_rows, 1, LANES)
    lane = iota(il, 2)
    lead = iota(il, 0)
    place = lane % half
    keep = (lane // half == lead % folds) & (
        (place // tile) * aminos + place % aminos == lead // folds)
    keep = jnp.where(keep, 1.0, 0.0)
    keep = jnp.broadcast_to(keep, (folds * pair_rows, low, LANES)).reshape(
        pair_rows * PROJ_FEATURES, LANES).astype(BF16).reshape(folds * pair_rows, low, LANES)

    for copy in left_copies:
        copy.wait_recv()
    product = jnp.zeros((pair_rows * PROJ_FEATURES, LANES), F32)
    for k in range(devices):
        right_k = dot(rep, right_buf[k]).astype(BF16)
        left_k = (left_buf[k][None] * keep).reshape(pair_rows * PROJ_FEATURES, LANES)
        product = product + dot(left_k, right_k)
    product_buf[...] = product
    for c in range(PROJ_FEATURES):
        slab = product_buf[pl.ds(c, pair_rows, stride=PROJ_FEATURES), :]
        lanes = iota((pair_rows, LANES), 1) // PROJ_FEATURES
        for j in range(aminos):
            lhs_buf[j * pair_rows:(j + 1) * pair_rows, c * per_c:(c + 1) * per_c] = jnp.where(
                lanes == j, slab, 0.0).astype(BF16)
    outer = dot(lhs_buf[...], weight_buf[...])
    result = (pair_turned + pair_mask * (outer / counts)).astype(BF16)
    pair_out_ref[...] = dot(order, result, 0, 0).astype(BF16)

    for copy in out_copies:
        copy.wait_recv()
    out_ref[...] = out_buf[...]
    for copy in emb_copies + aux_copies + left_copies + out_copies:
        copy.wait_send()


def fused(*args):
    emb, mask, resolved, pair = args[:4]
    groups, ranks = lax.axis_size("seq"), lax.axis_size("res")
    chains, aminos = emb.shape[:2]
    tile = chains // ranks * aminos
    pair_rows = pair.shape[0]
    devices = groups * ranks
    vmem = pl.BlockSpec(memory_space=pltpu.VMEM)
    dma = pltpu.SemaphoreType.DMA
    out, pair_out = pl.pallas_call(
        functools.partial(fused_kernel, groups, ranks, chains, aminos),
        out_shape=(
            jax.ShapeDtypeStruct((ranks, tile, ROW_FEATURES), BF16),
            jax.ShapeDtypeStruct((pair_rows * aminos, CZ), BF16),
        ),
        in_specs=[vmem] * 9,
        out_specs=(vmem, vmem),
        scratch_shapes=[
            pltpu.VMEM((ranks, tile, ROW_FEATURES), BF16),
            pltpu.VMEM((devices, 2 * HEAD_NUMBER, LANES), BF16),
            pltpu.VMEM((groups, tile, LANES), BF16),
            pltpu.VMEM((devices, tile, LANES), BF16),
            pltpu.VMEM((ranks, tile, LANES), BF16),
            pltpu.VMEM((devices, tile, LANES), BF16),
            pltpu.VMEM((ranks, tile, ROW_FEATURES), BF16),
            pltpu.VMEM((ranks, tile, ROW_FEATURES), BF16),
            pltpu.VMEM((PROJ_FEATURES * LANES, CZ), BF16),
            pltpu.VMEM((pair_rows * PROJ_FEATURES, LANES), F32),
            pltpu.VMEM((pair_rows * aminos, PROJ_FEATURES * LANES), BF16),
            dma((ranks,)), dma((ranks,)), dma((devices,)), dma((devices,)),
            dma((devices,)), dma((devices,)), dma((devices,)), dma((devices,)),
            dma((ranks,)), dma((ranks,)),
        ],
        compiler_params=pltpu.CompilerParams(collective_id=0, has_side_effects=True),
    )(
        emb.reshape(ranks, tile, ROW_FEATURES), mask, resolved.reshape(1, -1),
        pair.reshape(-1, CZ), *args[4:],
    )
    return out.reshape(emb.shape), pair_out.reshape(pair.shape)


def fits(mesh, emb, pair):
    groups, ranks = mesh.shape["seq"], mesh.shape["res"]
    chains, aminos = emb.shape[:2]
    if chains % ranks or aminos * PROJ_FEATURES != LANES or chains * aminos != LANES:
        return False
    pairs = pair.shape[0] * aminos
    return pairs * groups == LANES and chains // ranks * aminos * groups == PROJ_FEATURES


def solution(mesh):
    placed = (
        P(("crop", "seq"), "res", None),
        P(("crop", "seq"), "res"),
        P("crop"),
        P(("crop", "seq"), "res", None),
        P(),
        P(),
        P(),
        P(),
        P(),
    )
    def either(*args):
        return (fused if fits(mesh, args[0], args[3]) else per_device)(*args)

    return jax.shard_map(
        either,
        mesh=mesh,
        in_specs=placed,
        out_specs=(P(("crop", "seq"), "res", None), P(("crop", "seq"), "res", None)),
        check_vma=False,
    )
```

```python
import functools
import math

import jax
import jax.numpy as jnp
from jax import lax
from jax.experimental import pallas as pl
from jax.experimental.pallas import tpu as pltpu
from jax.sharding import PartitionSpec as P

ROW_FEATURES = 256
CZ = 128
HEAD_NUMBER = 8
PER_HEAD_DIM = 32
PROJ_FEATURES = 32


epsilon = 1e-05


def layer_normalize(values):
    values = values.astype(jnp.float32)
    average = jnp.mean(values, axis=-1, keepdims=True)
    centered = values - average
    variance = jnp.mean(centered * centered, axis=-1, keepdims=True)
    return centered * lax.rsqrt(variance + epsilon)


def outer_rows(left_side, right_side, project):
    row_total = left_side.shape[1]
    col_total = right_side.shape[1]
    block_rows = math.gcd(row_total, max(1, 2048 // col_total))

    def outer_block(start):
        product = jnp.einsum(
            "sic,sje->ijce", left_side, right_side, preferred_element_type=jnp.float32
        )
        flattened = product.reshape(block_rows * col_total, PROJ_FEATURES * PROJ_FEATURES)
        return jnp.dot(flattened, project, precision=lax.Precision.HIGHEST).reshape(
            block_rows, col_total, CZ
        )

    starts = jnp.arange(row_total // block_rows, dtype=jnp.int32) * block_rows
    return lax.map(outer_block, starts).reshape(row_total, col_total, CZ)


def per_device(
    aligned_chain_embedding,
    alignment_mask,
    resolved_residue_mask,
    pairwise_state,
    combined_projection_matrix,
    pair_bias_weight,
    final_projection_matrix,
    left_right_projection_matrix,
    outer_mean_weight,
):
    chain_count = aligned_chain_embedding.shape[0]
    amino_count = aligned_chain_embedding.shape[1]
    res_ranks = lax.axis_size("res")
    seq_groups = lax.axis_size("seq")
    full_length = amino_count * res_ranks
    row_count = full_length // seq_groups
    item_count = HEAD_NUMBER * chain_count // res_ranks
    per_head = min(item_count, chain_count)
    head_count = item_count // per_head
    my_rank = lax.axis_index("res")
    my_group = lax.axis_index("seq")
    standardized_rows = layer_normalize(aligned_chain_embedding).astype(jnp.bfloat16)
    linear_mapped = jnp.dot(
        standardized_rows.reshape(chain_count * amino_count, ROW_FEATURES),
        combined_projection_matrix,
        preferred_element_type=jnp.float32,
    )
    linear_mapped = linear_mapped.reshape(chain_count, amino_count, 4, HEAD_NUMBER, PER_HEAD_DIM)
    queries = (linear_mapped[:, :, 0] * PER_HEAD_DIM ** (-0.5)).astype(jnp.bfloat16)
    key_rows = linear_mapped[:, :, 1].astype(jnp.bfloat16)
    value_rows = linear_mapped[:, :, 2].astype(jnp.bfloat16)
    sigmoid_factor = jax.nn.sigmoid(linear_mapped[:, :, 3])
    stacked = jnp.stack([queries, key_rows, value_rows], axis=2)
    stacked = jnp.transpose(stacked, (3, 0, 1, 2, 4)).reshape(
        HEAD_NUMBER * chain_count, amino_count, 3 * PER_HEAD_DIM
    )
    presence_mask_flags = alignment_mask.astype(jnp.bfloat16)
    key_flags = jnp.broadcast_to(
        presence_mask_flags[None], (HEAD_NUMBER, chain_count, amino_count)
    ).reshape(HEAD_NUMBER * chain_count, amino_count)
    arrived, arrived_flags = (
        lax.all_to_all(stacked, "res", split_axis=0, concat_axis=1, tiled=True),
        lax.all_to_all(key_flags, "res", split_axis=0, concat_axis=1, tiled=True),
    )
    pair_normed = layer_normalize(pairwise_state).astype(jnp.bfloat16)
    local_bias = jnp.dot(
        pair_normed.reshape(row_count * amino_count, CZ),
        pair_bias_weight,
        preferred_element_type=jnp.float32,
    )
    local_bias = jnp.transpose(
        local_bias.astype(jnp.bfloat16).reshape(row_count, amino_count, HEAD_NUMBER), (2, 0, 1)
    )
    bias_cols = lax.all_gather(local_bias, "res", axis=2, tiled=True)
    whole_bias = lax.all_gather(bias_cols, "seq", axis=1, tiled=True)
    first_head = my_rank * item_count // chain_count
    head_bias = lax.dynamic_slice_in_dim(whole_bias, first_head, head_count, 0)
    grouped = arrived.reshape(head_count, per_head, full_length, 3, PER_HEAD_DIM)
    key_validity_mask = (
        arrived_flags.reshape(head_count, per_head, full_length).astype(jnp.float32) - 1.0
    ) * 1000000000.0
    scores = jnp.einsum(
        "gpid,gpjd->gpij",
        grouped[:, :, :, 0],
        grouped[:, :, :, 1],
        preferred_element_type=jnp.float32,
    )
    scores = scores + head_bias.astype(jnp.float32)[:, None] + key_validity_mask[:, :, None, :]
    row_max = jnp.max(scores, axis=-1, keepdims=True)
    exponent = jnp.exp(scores - row_max)
    weights = (exponent / jnp.sum(exponent, axis=-1, keepdims=True)).astype(jnp.bfloat16)
    softmax_mixed = jnp.einsum(
        "gpij,gpjd->gpid", weights, grouped[:, :, :, 2], preferred_element_type=jnp.float32
    )
    softmax_mixed = softmax_mixed.astype(jnp.bfloat16).reshape(
        item_count, full_length, PER_HEAD_DIM
    )
    returned = lax.all_to_all(softmax_mixed, "res", split_axis=1, concat_axis=0, tiled=True)
    returned = jnp.transpose(
        returned.reshape(HEAD_NUMBER, chain_count, amino_count, PER_HEAD_DIM), (1, 2, 0, 3)
    )
    sigmoid_scaled = (
        (sigmoid_factor * returned.astype(jnp.float32))
        .astype(jnp.bfloat16)
        .reshape(chain_count * amino_count, ROW_FEATURES)
    )
    embedding_increment = jnp.dot(
        sigmoid_scaled, final_projection_matrix, preferred_element_type=jnp.float32
    ).reshape(chain_count, amino_count, ROW_FEATURES)
    alignment_output = (aligned_chain_embedding.astype(jnp.float32) + embedding_increment).astype(
        jnp.bfloat16
    )
    standardized_product = layer_normalize(alignment_output).astype(jnp.bfloat16)
    left_right_vectors = jnp.dot(
        standardized_product.reshape(chain_count * amino_count, ROW_FEATURES),
        left_right_projection_matrix,
        preferred_element_type=jnp.float32,
    )
    left_right_vectors = left_right_vectors.reshape(chain_count, amino_count, 2, PROJ_FEATURES)
    entry_present = alignment_mask.astype(jnp.float32)[:, :, None]
    left_side = (left_right_vectors[:, :, 0] * entry_present).astype(jnp.bfloat16)
    right_side = (left_right_vectors[:, :, 1] * entry_present).astype(jnp.bfloat16)
    left_all, left_flags = (
        lax.all_gather(left_side, "res", axis=1, tiled=True),
        lax.all_gather(presence_mask_flags, "res", axis=1, tiled=True),
    )
    project = outer_mean_weight.astype(jnp.float32)
    row_start = my_group * row_count
    left_full, flag_full = (
        lax.all_to_all(left_all, "seq", split_axis=1, concat_axis=0, tiled=True),
        lax.all_to_all(left_flags, "seq", split_axis=1, concat_axis=0, tiled=True),
    )
    right_full, right_flags = (
        lax.all_gather(right_side, "seq", axis=0, tiled=True),
        lax.all_gather(presence_mask_flags, "seq", axis=0, tiled=True),
    )
    counts = jnp.dot(flag_full.T, right_flags, preferred_element_type=jnp.float32)
    outer = outer_rows(left_full, right_full, project)
    col_start = my_rank * amino_count
    row_mask = lax.dynamic_slice_in_dim(resolved_residue_mask, row_start, row_count).astype(
        jnp.float32
    )
    col_mask = lax.dynamic_slice_in_dim(resolved_residue_mask, col_start, amino_count).astype(
        jnp.float32
    )
    pair_mask = row_mask[:, None] * col_mask[None, :]
    pairwise_output = (
        pairwise_state.astype(jnp.float32) + pair_mask[:, :, None] * (outer / counts[:, :, None])
    ).astype(jnp.bfloat16)
    return (alignment_output, pairwise_output)


LANES = 128
F32 = jnp.float32
BF16 = jnp.bfloat16


def iota(shape, axis):
    return lax.broadcasted_iota(jnp.int32, shape, axis)


def dot(a, b, ca=1, cb=0):
    return lax.dot_general(a, b, (((ca,), (cb,)), ((), ())), preferred_element_type=F32)


def one_hot(cond):
    return jnp.where(cond, 1.0, 0.0).astype(BF16)


def fused_kernel(
    groups, ranks, chains, aminos,
    emb_ref, mask_ref, resolved_ref, pair_ref, proj_ref, bias_w_ref, final_ref, lr_ref, outer_ref,
    out_ref, pair_out_ref,
    emb_buf, aux_buf, left_send, left_buf, right_send, right_buf, out_send, out_buf,
    product_buf, lhs_buf,
    emb_s, emb_r, aux_s, aux_r, left_s, left_r, right_s, right_r, out_s, out_r,
):
    devices = groups * ranks
    per = chains // ranks
    tile = per * aminos
    rows = ranks * tile
    full = ranks * aminos
    pair_rows = full // groups
    pairs = pair_rows * aminos
    half = rows // groups
    group = lax.axis_index("seq")
    rank = lax.axis_index("res")
    me = group * ranks + rank

    def peer_of(k):
        peer = lax.rem(me + k, devices)
        return peer, {"seq": peer // ranks, "res": lax.rem(peer, ranks)}

    barrier = pltpu.get_barrier_semaphore()
    for k in range(1, devices):
        pl.semaphore_signal(
            barrier, inc=1, device_id=peer_of(k)[1], device_id_type=pl.DeviceIdType.MESH
        )

    def send(src, dst, ssem, rsem, device):
        copy = pltpu.make_async_remote_copy(
            src_ref=src, dst_ref=dst, send_sem=ssem, recv_sem=rsem,
            device_id=device, device_id_type=pl.DeviceIdType.MESH,
        )
        copy.start()
        return copy

    pair_value = pair_ref[...]
    pair_normed = layer_normalize(pair_value).astype(BF16)
    wide = jnp.concatenate([pair_normed] * groups, axis=0)
    wide = jnp.where(iota((groups * pairs, CZ), 0) // pairs == group, wide, jnp.zeros_like(wide))
    own_bias = dot(bias_w_ref[...], wide, 1, 1)
    spread = dot(mask_ref[...].astype(F32).astype(BF16), one_hot(
        iota((chains, LANES), 1) // aminos == iota((chains, LANES), 0)))
    flag_row = jnp.sum(
        jnp.where(iota((aminos, LANES), 1) % aminos == iota((aminos, LANES), 0), spread, 0.0),
        axis=0, keepdims=True)
    flags = jnp.broadcast_to(flag_row, (HEAD_NUMBER, LANES))
    aux_buf[me] = jnp.concatenate([own_bias, flags], axis=0).astype(BF16)
    own = pl.ds(rank * per, per)
    emb_buf[own] = emb_ref[own]

    pl.semaphore_wait(barrier, devices - 1)
    pending = []
    emb_copies = []
    for k in range(1, ranks):
        peer = lax.rem(rank + k, ranks)
        emb_copies.append(send(emb_ref.at[pl.ds(peer * per, per)], emb_buf.at[own],
                               emb_s.at[k], emb_r.at[k],
                               {"seq": group, "res": peer}))
    aux_copies = []
    for k in range(1, devices):
        aux_copies.append(send(aux_buf.at[me], aux_buf.at[me], aux_s.at[k], aux_r.at[k],
                               peer_of(k)[1]))

    quads = pair_rows // aminos

    def row_of(q):
        return (q % quads) * aminos + (q % pair_rows) // quads

    q0 = iota((pairs, pairs), 0)
    q1 = iota((pairs, pairs), 1)
    order = one_hot(row_of(q0) * aminos + q0 // pair_rows == q1)
    pair_turned = dot(order, pair_value)
    lane_r = iota((pairs, full), 1)
    row_r = iota((pairs, full), 0)
    resolved = jnp.broadcast_to(resolved_ref[...].astype(F32), (pairs, full))
    pair_mask = jnp.sum(
        jnp.where(lane_r == group * pair_rows + row_of(row_r), resolved, 0.0),
        axis=1, keepdims=True
    ) * jnp.sum(
        jnp.where(lane_r == rank * aminos + row_r // pair_rows, resolved, 0.0),
        axis=1, keepdims=True)

    for copy in emb_copies:
        copy.wait_recv()
    embedding = emb_buf[...].astype(F32).reshape(rows, ROW_FEATURES)
    normed = layer_normalize(embedding).astype(BF16)
    projected = dot(normed, proj_ref[...])
    width = HEAD_NUMBER * PER_HEAD_DIM
    queries = (projected[:, :width] * PER_HEAD_DIM ** (-0.5)).astype(BF16)
    keys = projected[:, width:2 * width].astype(BF16)
    values = projected[:, 2 * width:3 * width].astype(BF16)
    gating = jax.nn.sigmoid(projected[:, 3 * width:])

    for copy in aux_copies:
        copy.wait_recv()
    aux = aux_buf[...].astype(F32)
    bias_all = aux[0:ranks, :HEAD_NUMBER]
    for g in range(1, groups):
        bias_all = bias_all + aux[g * ranks:(g + 1) * ranks, :HEAD_NUMBER]
    bias_all = bias_all.reshape(ranks * HEAD_NUMBER, LANES).astype(BF16)
    hq = (HEAD_NUMBER * rows, ranks * HEAD_NUMBER)
    pick = one_hot(
        ((iota(hq, 0) % rows) // tile) * HEAD_NUMBER + iota(hq, 0) // rows == iota(hq, 1))
    bias_q = dot(pick, bias_all)
    hl = (HEAD_NUMBER * rows, LANES)
    bias_q = jnp.where(iota(hl, 1) % aminos == iota(hl, 0) % aminos, bias_q, 0.0).astype(BF16)
    pp = iota((rows, LANES), 0)
    ll = iota((rows, LANES), 1)
    row_pick = one_hot(ll // aminos == (pp // tile) * aminos + pp % aminos)
    bias_full = dot(row_pick, bias_q, 1, 1)
    flag_all = aux[:, HEAD_NUMBER:HEAD_NUMBER + 1].reshape(devices, LANES).astype(BF16)
    near = dot(flag_all, one_hot(pp == rank * tile + ll % tile))
    near_row = jnp.sum(
        jnp.where(
            iota((devices, LANES), 0) == group * ranks + iota((devices, LANES), 1) // tile,
            near, 0.0),
        axis=0, keepdims=True)
    key_mask = (near_row - 1.0) * 1000000000.0
    present = jnp.sum(jnp.where(pp == ll, near_row, 0.0), axis=1, keepdims=True)
    same_chain = (pp // aminos) % per == (ll // aminos) % per
    heads_per = LANES // PER_HEAD_DIM
    mixed = []
    for block in range(width // LANES):
        cols = slice(block * LANES, (block + 1) * LANES)
        total = jnp.zeros((rows, LANES), F32)
        for sub in range(heads_per):
            head = block * heads_per + sub
            lanes = ll // PER_HEAD_DIM == sub
            query = jnp.where(lanes, queries[:, cols], jnp.zeros((), BF16))
            scores = dot(query, keys[:, cols], 1, 1)
            scores = scores + bias_full[:, head * rows:(head + 1) * rows] + key_mask
            scores = jnp.where(same_chain, scores, -3e38)
            exponent = jnp.exp(scores - jnp.max(scores, axis=1, keepdims=True))
            weights = (exponent / jnp.sum(exponent, axis=1, keepdims=True)).astype(BF16)
            total = jnp.where(lanes, dot(weights, values[:, cols]), total)
        mixed.append(total)
    attended = jnp.concatenate(mixed, axis=1).astype(BF16)
    gated = (gating * attended.astype(F32)).astype(BF16)
    updated = (embedding + dot(gated, final_ref[...])).astype(BF16)
    normed_out = layer_normalize(updated).astype(BF16)

    left_w = jnp.concatenate([lr_ref[:PROJ_FEATURES, :]] * quads, axis=0)
    right_w = jnp.concatenate([lr_ref[PROJ_FEATURES:, :]] * aminos, axis=0)
    left = dot(normed_out, left_w, 1, 1) * present
    left = jnp.where(ll // PROJ_FEATURES == (pp // tile) % quads, left, 0.0)
    for g in range(groups):
        part = left[g * half:g * half + tile]
        for r in range(1, quads):
            part = part + left[g * half + r * tile:g * half + (r + 1) * tile]
        left_send[g] = part.astype(BF16)
    right = dot(normed_out, right_w, 1, 1) * present
    right = jnp.where(ll // PROJ_FEATURES == pp % aminos, right, 0.0).astype(BF16)
    right_send[...] = right.reshape(ranks, tile, LANES)
    out_send[...] = updated.astype(F32).reshape(chains, aminos, ROW_FEATURES).astype(BF16)
    left_copies = []
    for k in range(1, devices):
        peer, device = peer_of(k)
        left_copies.append(send(left_send.at[peer // ranks], left_buf.at[me],
                                left_s.at[k], left_r.at[k], device))
        left_copies.append(send(right_send.at[lax.rem(peer, ranks)], right_buf.at[me],
                                right_s.at[k], right_r.at[k], device))
    out_copies = []
    for k in range(1, ranks):
        peer = lax.rem(rank + k, ranks)
        out_copies.append(send(out_send.at[pl.ds(peer * per, per)], out_buf.at[own], out_s.at[k], out_r.at[k],
                               {"seq": group, "res": peer}))
    left_buf[me] = left_send[group]
    right_buf[me] = right_send[rank]
    out_buf[own] = out_send[own]

    gq = (groups * pairs, devices)
    gl = (groups * pairs, LANES)
    within = iota(gl, 0) % pairs
    row_at = group * pair_rows + row_of(within)
    group_q = iota(gq, 0) // pairs
    row_at_q = group * pair_rows + row_of(iota(gq, 0) % pairs)
    row_flags = dot(one_hot(group_q * ranks + row_at_q // aminos == iota(gq, 1)), flag_all)
    col_flags = dot(one_hot(group_q * ranks + rank == iota(gq, 1)), flag_all)
    amino_l = iota(gl, 1) % aminos
    gather_s = one_hot(pp // aminos == ll)
    row_flags = dot(one_hot((amino_l == row_at % aminos) & (row_flags > 0.5)), gather_s)
    col_flags = dot(one_hot((amino_l == within // pair_rows) & (col_flags > 0.5)), gather_s)
    both = jnp.sum(row_flags * col_flags, axis=1, keepdims=True)
    counts = both[:pairs]
    for g in range(1, groups):
        counts = counts + both[g * pairs:(g + 1) * pairs]

    depth = devices * tile
    rep = one_hot(iota((depth, depth), 0) // aminos == iota((depth, depth), 1) // aminos)
    amino_d = iota((depth, LANES), 0) % aminos
    block = iota((pair_rows, LANES), 1) // PROJ_FEATURES
    for copy in left_copies:
        copy.wait_recv()
    left_all = left_buf[...].reshape(depth, LANES)
    right_all = dot(rep, right_buf[...].reshape(depth, LANES))
    right_all = jnp.concatenate(
        [jnp.where(amino_d == a, right_all, 0.0).astype(BF16) for a in range(aminos)], axis=1)
    product = dot(left_all, right_all, 0, 0)
    for a in range(aminos):
        product_buf[a * LANES:(a + 1) * LANES, :] = product[:, a * LANES:(a + 1) * LANES]
    for c in range(0, PROJ_FEATURES, aminos):
        slabs = [product_buf[pl.ds(c + x, pair_rows, stride=PROJ_FEATURES), :]
                 for x in range(aminos)]
        for j in range(aminos):
            turned = jnp.zeros((pair_rows, LANES), F32)
            for x in range(aminos):
                shift = (x - j) % aminos * PROJ_FEATURES
                moved = pltpu.roll(slabs[x], shift, 1) if shift else slabs[x]
                turned = jnp.where(block == x, moved, turned)
            lhs_buf[j * pair_rows:(j + 1) * pair_rows,
                    c * PROJ_FEATURES:c * PROJ_FEATURES + LANES] = turned.astype(BF16)
    outer = dot(lhs_buf[...], outer_ref[...])
    result = (pair_turned + pair_mask * (outer / counts)).astype(BF16)
    pair_out_ref[...] = dot(order, result, 0, 0).astype(BF16)

    for copy in out_copies:
        copy.wait_recv()
    out_ref[...] = out_buf[...]
    for copy in emb_copies + aux_copies + left_copies + out_copies:
        copy.wait_send()


def fused(*args):
    emb, mask, resolved, pair = args[:4]
    groups, ranks = lax.axis_size("seq"), lax.axis_size("res")
    chains, aminos = emb.shape[:2]
    tile = chains // ranks * aminos
    pair_rows = pair.shape[0]
    devices = groups * ranks
    vmem = pl.BlockSpec(memory_space=pltpu.VMEM)
    dma = pltpu.SemaphoreType.DMA
    out, pair_out = pl.pallas_call(
        functools.partial(fused_kernel, groups, ranks, chains, aminos),
        out_shape=(
            jax.ShapeDtypeStruct(emb.shape, BF16),
            jax.ShapeDtypeStruct((pair_rows * aminos, CZ), BF16),
        ),
        in_specs=[vmem] * 9,
        out_specs=(vmem, vmem),
        scratch_shapes=[
            pltpu.VMEM(emb.shape, BF16),
            pltpu.VMEM((devices, 2 * HEAD_NUMBER, LANES), BF16),
            pltpu.VMEM((groups, tile, LANES), BF16),
            pltpu.VMEM((devices, tile, LANES), BF16),
            pltpu.VMEM((ranks, tile, LANES), BF16),
            pltpu.VMEM((devices, tile, LANES), BF16),
            pltpu.VMEM(emb.shape, BF16),
            pltpu.VMEM(emb.shape, BF16),
            pltpu.VMEM((pair_rows * PROJ_FEATURES, LANES), F32),
            pltpu.VMEM((pair_rows * aminos, PROJ_FEATURES * PROJ_FEATURES), BF16),
            dma((ranks,)), dma((ranks,)), dma((devices,)), dma((devices,)),
            dma((devices,)), dma((devices,)), dma((devices,)), dma((devices,)),
            dma((ranks,)), dma((ranks,)),
        ],
        compiler_params=pltpu.CompilerParams(collective_id=0, has_side_effects=True),
    )(
        emb, mask.T, resolved.reshape(1, -1),
        pair.reshape(-1, CZ), args[4], args[5].T, args[6], args[7].T, args[8],
    )
    return out, pair_out.reshape(pair.shape)


def fits(mesh, emb, pair):
    groups, ranks = mesh.shape["seq"], mesh.shape["res"]
    chains, aminos = emb.shape[:2]
    if chains % ranks or aminos * PROJ_FEATURES != LANES or chains * aminos != LANES:
        return False
    pairs = pair.shape[0] * aminos
    return pairs * groups == LANES and chains // ranks * aminos * groups == PROJ_FEATURES


def solution(mesh):
    placed = (
        P(("crop", "seq"), "res", None),
        P(("crop", "seq"), "res"),
        P("crop"),
        P(("crop", "seq"), "res", None),
        P(),
        P(),
        P(),
        P(),
        P(),
    )
    def either(*args):
        return (fused if fits(mesh, args[0], args[3]) else per_device)(*args)

    return jax.shard_map(
        either,
        mesh=mesh,
        in_specs=placed,
        out_specs=(P(("crop", "seq"), "res", None), P(("crop", "seq"), "res", None)),
        check_vma=False,
    )
```

```python
import functools
import math

import jax
import jax.numpy as jnp
from jax import lax
from jax.experimental import pallas as pl
from jax.experimental.pallas import tpu as pltpu
from jax.sharding import PartitionSpec as P

ROW_FEATURES = 256
CZ = 128
HEAD_NUMBER = 8
PER_HEAD_DIM = 32
PROJ_FEATURES = 32


epsilon = 1e-05


def layer_normalize(values):
    values = values.astype(jnp.float32)
    average = jnp.mean(values, axis=-1, keepdims=True)
    centered = values - average
    variance = jnp.mean(centered * centered, axis=-1, keepdims=True)
    return centered * lax.rsqrt(variance + epsilon)


def outer_rows(left_side, right_side, project):
    row_total = left_side.shape[1]
    col_total = right_side.shape[1]
    block_rows = math.gcd(row_total, max(1, 2048 // col_total))

    def outer_block(start):
        product = jnp.einsum(
            "sic,sje->ijce", left_side, right_side, preferred_element_type=jnp.float32
        )
        flattened = product.reshape(block_rows * col_total, PROJ_FEATURES * PROJ_FEATURES)
        return jnp.dot(flattened, project, precision=lax.Precision.HIGHEST).reshape(
            block_rows, col_total, CZ
        )

    starts = jnp.arange(row_total // block_rows, dtype=jnp.int32) * block_rows
    return lax.map(outer_block, starts).reshape(row_total, col_total, CZ)


def per_device(
    aligned_chain_embedding,
    alignment_mask,
    resolved_residue_mask,
    pairwise_state,
    combined_projection_matrix,
    pair_bias_weight,
    final_projection_matrix,
    left_right_projection_matrix,
    outer_mean_weight,
):
    chain_count = aligned_chain_embedding.shape[0]
    amino_count = aligned_chain_embedding.shape[1]
    res_ranks = lax.axis_size("res")
    seq_groups = lax.axis_size("seq")
    full_length = amino_count * res_ranks
    row_count = full_length // seq_groups
    item_count = HEAD_NUMBER * chain_count // res_ranks
    per_head = min(item_count, chain_count)
    head_count = item_count // per_head
    my_rank = lax.axis_index("res")
    my_group = lax.axis_index("seq")
    standardized_rows = layer_normalize(aligned_chain_embedding).astype(jnp.bfloat16)
    linear_mapped = jnp.dot(
        standardized_rows.reshape(chain_count * amino_count, ROW_FEATURES),
        combined_projection_matrix,
        preferred_element_type=jnp.float32,
    )
    linear_mapped = linear_mapped.reshape(chain_count, amino_count, 4, HEAD_NUMBER, PER_HEAD_DIM)
    queries = (linear_mapped[:, :, 0] * PER_HEAD_DIM ** (-0.5)).astype(jnp.bfloat16)
    key_rows = linear_mapped[:, :, 1].astype(jnp.bfloat16)
    value_rows = linear_mapped[:, :, 2].astype(jnp.bfloat16)
    sigmoid_factor = jax.nn.sigmoid(linear_mapped[:, :, 3])
    stacked = jnp.stack([queries, key_rows, value_rows], axis=2)
    stacked = jnp.transpose(stacked, (3, 0, 1, 2, 4)).reshape(
        HEAD_NUMBER * chain_count, amino_count, 3 * PER_HEAD_DIM
    )
    presence_mask_flags = alignment_mask.astype(jnp.bfloat16)
    key_flags = jnp.broadcast_to(
        presence_mask_flags[None], (HEAD_NUMBER, chain_count, amino_count)
    ).reshape(HEAD_NUMBER * chain_count, amino_count)
    arrived, arrived_flags = (
        lax.all_to_all(stacked, "res", split_axis=0, concat_axis=1, tiled=True),
        lax.all_to_all(key_flags, "res", split_axis=0, concat_axis=1, tiled=True),
    )
    pair_normed = layer_normalize(pairwise_state).astype(jnp.bfloat16)
    local_bias = jnp.dot(
        pair_normed.reshape(row_count * amino_count, CZ),
        pair_bias_weight,
        preferred_element_type=jnp.float32,
    )
    local_bias = jnp.transpose(
        local_bias.astype(jnp.bfloat16).reshape(row_count, amino_count, HEAD_NUMBER), (2, 0, 1)
    )
    bias_cols = lax.all_gather(local_bias, "res", axis=2, tiled=True)
    whole_bias = lax.all_gather(bias_cols, "seq", axis=1, tiled=True)
    first_head = my_rank * item_count // chain_count
    head_bias = lax.dynamic_slice_in_dim(whole_bias, first_head, head_count, 0)
    grouped = arrived.reshape(head_count, per_head, full_length, 3, PER_HEAD_DIM)
    key_validity_mask = (
        arrived_flags.reshape(head_count, per_head, full_length).astype(jnp.float32) - 1.0
    ) * 1000000000.0
    scores = jnp.einsum(
        "gpid,gpjd->gpij",
        grouped[:, :, :, 0],
        grouped[:, :, :, 1],
        preferred_element_type=jnp.float32,
    )
    scores = scores + head_bias.astype(jnp.float32)[:, None] + key_validity_mask[:, :, None, :]
    row_max = jnp.max(scores, axis=-1, keepdims=True)
    exponent = jnp.exp(scores - row_max)
    weights = (exponent / jnp.sum(exponent, axis=-1, keepdims=True)).astype(jnp.bfloat16)
    softmax_mixed = jnp.einsum(
        "gpij,gpjd->gpid", weights, grouped[:, :, :, 2], preferred_element_type=jnp.float32
    )
    softmax_mixed = softmax_mixed.astype(jnp.bfloat16).reshape(
        item_count, full_length, PER_HEAD_DIM
    )
    returned = lax.all_to_all(softmax_mixed, "res", split_axis=1, concat_axis=0, tiled=True)
    returned = jnp.transpose(
        returned.reshape(HEAD_NUMBER, chain_count, amino_count, PER_HEAD_DIM), (1, 2, 0, 3)
    )
    sigmoid_scaled = (
        (sigmoid_factor * returned.astype(jnp.float32))
        .astype(jnp.bfloat16)
        .reshape(chain_count * amino_count, ROW_FEATURES)
    )
    embedding_increment = jnp.dot(
        sigmoid_scaled, final_projection_matrix, preferred_element_type=jnp.float32
    ).reshape(chain_count, amino_count, ROW_FEATURES)
    alignment_output = (aligned_chain_embedding.astype(jnp.float32) + embedding_increment).astype(
        jnp.bfloat16
    )
    standardized_product = layer_normalize(alignment_output).astype(jnp.bfloat16)
    left_right_vectors = jnp.dot(
        standardized_product.reshape(chain_count * amino_count, ROW_FEATURES),
        left_right_projection_matrix,
        preferred_element_type=jnp.float32,
    )
    left_right_vectors = left_right_vectors.reshape(chain_count, amino_count, 2, PROJ_FEATURES)
    entry_present = alignment_mask.astype(jnp.float32)[:, :, None]
    left_side = (left_right_vectors[:, :, 0] * entry_present).astype(jnp.bfloat16)
    right_side = (left_right_vectors[:, :, 1] * entry_present).astype(jnp.bfloat16)
    left_all, left_flags = (
        lax.all_gather(left_side, "res", axis=1, tiled=True),
        lax.all_gather(presence_mask_flags, "res", axis=1, tiled=True),
    )
    project = outer_mean_weight.astype(jnp.float32)
    row_start = my_group * row_count
    left_full, flag_full = (
        lax.all_to_all(left_all, "seq", split_axis=1, concat_axis=0, tiled=True),
        lax.all_to_all(left_flags, "seq", split_axis=1, concat_axis=0, tiled=True),
    )
    right_full, right_flags = (
        lax.all_gather(right_side, "seq", axis=0, tiled=True),
        lax.all_gather(presence_mask_flags, "seq", axis=0, tiled=True),
    )
    counts = jnp.dot(flag_full.T, right_flags, preferred_element_type=jnp.float32)
    outer = outer_rows(left_full, right_full, project)
    col_start = my_rank * amino_count
    row_mask = lax.dynamic_slice_in_dim(resolved_residue_mask, row_start, row_count).astype(
        jnp.float32
    )
    col_mask = lax.dynamic_slice_in_dim(resolved_residue_mask, col_start, amino_count).astype(
        jnp.float32
    )
    pair_mask = row_mask[:, None] * col_mask[None, :]
    pairwise_output = (
        pairwise_state.astype(jnp.float32) + pair_mask[:, :, None] * (outer / counts[:, :, None])
    ).astype(jnp.bfloat16)
    return (alignment_output, pairwise_output)


LANES = 128
F32 = jnp.float32
BF16 = jnp.bfloat16


def iota(shape, axis):
    return lax.broadcasted_iota(jnp.int32, shape, axis)


def dot(a, b, ca=1, cb=0):
    return lax.dot_general(a, b, (((ca,), (cb,)), ((), ())), preferred_element_type=F32)


def one_hot(cond):
    return jnp.where(cond, 1.0, 0.0).astype(BF16)


def fused_kernel(
    groups, ranks, chains, aminos,
    emb_ref, mask_ref, resolved_ref, pair_ref, proj_hbm, bias_w_ref, final_hbm, lr_ref, outer_hbm,
    out_ref, pair_out_ref,
    emb_buf, aux_buf, side_send, side_buf, out_send, out_buf,
    product_buf, lhs_buf, proj_ref, final_ref, outer_ref,
    emb_s, emb_r, aux_s, aux_r, side_s, side_r, out_s, out_r, load_s,
):
    devices = groups * ranks
    per = chains // ranks
    tile = per * aminos
    rows = ranks * tile
    full = ranks * aminos
    pair_rows = full // groups
    pairs = pair_rows * aminos
    half = rows // groups
    group = lax.axis_index("seq")
    rank = lax.axis_index("res")
    me = group * ranks + rank

    def peer_of(k):
        peer = lax.rem(me + k, devices)
        return peer, {"seq": peer // ranks, "res": lax.rem(peer, ranks)}

    barrier = pltpu.get_barrier_semaphore()
    for k in range(1, devices):
        pl.semaphore_signal(
            barrier, inc=1, device_id=peer_of(k)[1], device_id_type=pl.DeviceIdType.MESH
        )

    loads = []
    for k, (src, dst) in enumerate(
        ((proj_hbm, proj_ref), (final_hbm, final_ref), (outer_hbm, outer_ref))
    ):
        loads.append(pltpu.make_async_copy(src, dst, load_s.at[k]))
        loads[-1].start()

    def send(src, dst, ssem, rsem, device):
        copy = pltpu.make_async_remote_copy(
            src_ref=src, dst_ref=dst, send_sem=ssem, recv_sem=rsem,
            device_id=device, device_id_type=pl.DeviceIdType.MESH,
        )
        copy.start()
        return copy

    pair_value = pair_ref[...]
    pair_normed = layer_normalize(pair_value).astype(BF16)
    wide = jnp.concatenate([pair_normed] * groups, axis=0)
    wide = jnp.where(iota((groups * pairs, CZ), 0) // pairs == group, wide, jnp.zeros_like(wide))
    own_bias = dot(bias_w_ref[...], wide, 1, 1)
    spread = dot(mask_ref[...].astype(F32).astype(BF16), one_hot(
        iota((chains, LANES), 1) // aminos == iota((chains, LANES), 0)))
    flag_row = jnp.sum(
        jnp.where(iota((aminos, LANES), 1) % aminos == iota((aminos, LANES), 0), spread, 0.0),
        axis=0, keepdims=True)
    flags = jnp.broadcast_to(flag_row, (HEAD_NUMBER, LANES))
    aux_buf[me] = jnp.concatenate([own_bias, flags], axis=0).astype(BF16)
    own = pl.ds(rank * per, per)
    emb_buf[own] = emb_ref[own]

    pl.semaphore_wait(barrier, devices - 1)
    pending = []
    emb_copies = []
    for k in range(1, ranks):
        peer = lax.rem(rank + k, ranks)
        emb_copies.append(send(emb_ref.at[pl.ds(peer * per, per)], emb_buf.at[own],
                               emb_s.at[k], emb_r.at[k],
                               {"seq": group, "res": peer}))
    aux_copies = []
    for k in range(1, devices):
        aux_copies.append(send(aux_buf.at[me], aux_buf.at[me], aux_s.at[k], aux_r.at[k],
                               peer_of(k)[1]))

    quads = pair_rows // aminos

    def row_of(q):
        return (q % quads) * aminos + (q % pair_rows) // quads

    q0 = iota((pairs, pairs), 0)
    q1 = iota((pairs, pairs), 1)
    order = one_hot(row_of(q0) * aminos + q0 // pair_rows == q1)
    pair_turned = dot(order, pair_value)
    lane_r = iota((pairs, full), 1)
    row_r = iota((pairs, full), 0)
    resolved = jnp.broadcast_to(resolved_ref[...].astype(F32), (pairs, full))
    pair_mask = jnp.sum(
        jnp.where(lane_r == group * pair_rows + row_of(row_r), resolved, 0.0),
        axis=1, keepdims=True
    ) * jnp.sum(
        jnp.where(lane_r == rank * aminos + row_r // pair_rows, resolved, 0.0),
        axis=1, keepdims=True)

    for copy in emb_copies:
        copy.wait_recv()
    embedding = emb_buf[...].astype(F32).reshape(rows, ROW_FEATURES)
    normed = layer_normalize(embedding).astype(BF16)
    loads[0].wait()
    projected = dot(normed, proj_ref[...])
    width = HEAD_NUMBER * PER_HEAD_DIM
    queries = (projected[:, :width] * PER_HEAD_DIM ** (-0.5)).astype(BF16)
    keys = projected[:, width:2 * width].astype(BF16)
    values = projected[:, 2 * width:3 * width].astype(BF16)
    gating = jax.nn.sigmoid(projected[:, 3 * width:])

    for copy in aux_copies:
        copy.wait_recv()
    aux = aux_buf[...].astype(F32)
    bias_all = aux[0:ranks, :HEAD_NUMBER]
    for g in range(1, groups):
        bias_all = bias_all + aux[g * ranks:(g + 1) * ranks, :HEAD_NUMBER]
    bias_all = bias_all.reshape(ranks * HEAD_NUMBER, LANES).astype(BF16)
    hq = (HEAD_NUMBER * rows, ranks * HEAD_NUMBER)
    pick = one_hot(
        ((iota(hq, 0) % rows) // tile) * HEAD_NUMBER + iota(hq, 0) // rows == iota(hq, 1))
    bias_q = dot(pick, bias_all)
    hl = (HEAD_NUMBER * rows, LANES)
    bias_q = jnp.where(iota(hl, 1) % aminos == iota(hl, 0) % aminos, bias_q, 0.0).astype(BF16)
    pp = iota((rows, LANES), 0)
    ll = iota((rows, LANES), 1)
    row_pick = one_hot(ll // aminos == (pp // tile) * aminos + pp % aminos)
    bias_full = dot(row_pick, bias_q, 1, 1)
    flag_all = aux[:, HEAD_NUMBER:HEAD_NUMBER + 1].reshape(devices, LANES).astype(BF16)
    near = dot(flag_all, one_hot(pp == rank * tile + ll % tile))
    near_row = jnp.sum(
        jnp.where(
            iota((devices, LANES), 0) == group * ranks + iota((devices, LANES), 1) // tile,
            near, 0.0),
        axis=0, keepdims=True)
    key_mask = (near_row - 1.0) * 1000000000.0
    present = jnp.sum(jnp.where(pp == ll, near_row, 0.0), axis=1, keepdims=True)
    same_chain = (pp // aminos) % per == (ll // aminos) % per
    heads_per = LANES // PER_HEAD_DIM
    mixed = []
    for block in range(width // LANES):
        cols = slice(block * LANES, (block + 1) * LANES)
        total = jnp.zeros((rows, LANES), F32)
        for sub in range(heads_per):
            head = block * heads_per + sub
            lanes = ll // PER_HEAD_DIM == sub
            query = jnp.where(lanes, queries[:, cols], jnp.zeros((), BF16))
            scores = dot(query, keys[:, cols], 1, 1)
            scores = scores + bias_full[:, head * rows:(head + 1) * rows] + key_mask
            scores = jnp.where(same_chain, scores, -3e38)
            exponent = jnp.exp(scores - jnp.max(scores, axis=1, keepdims=True))
            weights = (exponent / jnp.sum(exponent, axis=1, keepdims=True)).astype(BF16)
            total = jnp.where(lanes, dot(weights, values[:, cols]), total)
        mixed.append(total)
    attended = jnp.concatenate(mixed, axis=1).astype(BF16)
    gated = (gating * attended.astype(F32)).astype(BF16)
    loads[1].wait()
    updated = (embedding + dot(gated, final_ref[...])).astype(BF16)
    normed_out = layer_normalize(updated).astype(BF16)

    left_w = jnp.concatenate([lr_ref[:PROJ_FEATURES, :]] * quads, axis=0)
    right_w = jnp.concatenate([lr_ref[PROJ_FEATURES:, :]] * aminos, axis=0)
    left = dot(normed_out, left_w, 1, 1) * present
    left = jnp.where(ll // PROJ_FEATURES == (pp // tile) % quads, left, 0.0)
    for g in range(groups):
        part = left[g * half:g * half + tile]
        for r in range(1, quads):
            part = part + left[g * half + r * tile:g * half + (r + 1) * tile]
        for r in range(ranks):
            side_send[g * ranks + r, :tile] = part.astype(BF16)
    right = dot(normed_out, right_w, 1, 1) * present
    right = jnp.where(ll // PROJ_FEATURES == pp % aminos, right, 0.0).astype(BF16)
    for d in range(devices):
        at = d % ranks * tile
        side_send[d, tile:] = right[at:at + tile]
    out_send[...] = updated.astype(F32).reshape(chains, aminos, ROW_FEATURES).astype(BF16)
    left_copies = []
    for k in range(1, devices):
        peer, device = peer_of(k)
        left_copies.append(send(side_send.at[peer], side_buf.at[me], side_s.at[k], side_r.at[k],
                                device))
    out_copies = []
    for k in range(1, ranks):
        peer = lax.rem(rank + k, ranks)
        out_copies.append(send(out_send.at[pl.ds(peer * per, per)], out_buf.at[own], out_s.at[k], out_r.at[k],
                               {"seq": group, "res": peer}))
    side_buf[me] = side_send[me]
    out_buf[own] = out_send[own]

    gq = (groups * pairs, devices)
    gl = (groups * pairs, LANES)
    within = iota(gl, 0) % pairs
    row_at = group * pair_rows + row_of(within)
    group_q = iota(gq, 0) // pairs
    row_at_q = group * pair_rows + row_of(iota(gq, 0) % pairs)
    row_flags = dot(one_hot(group_q * ranks + row_at_q // aminos == iota(gq, 1)), flag_all)
    col_flags = dot(one_hot(group_q * ranks + rank == iota(gq, 1)), flag_all)
    amino_l = iota(gl, 1) % aminos
    gather_s = one_hot(pp // aminos == ll)
    row_flags = dot(one_hot((amino_l == row_at % aminos) & (row_flags > 0.5)), gather_s)
    col_flags = dot(one_hot((amino_l == within // pair_rows) & (col_flags > 0.5)), gather_s)
    both = jnp.sum(row_flags * col_flags, axis=1, keepdims=True)
    counts = both[:pairs]
    for g in range(1, groups):
        counts = counts + both[g * pairs:(g + 1) * pairs]

    depth = devices * tile
    rep = one_hot(iota((depth, depth), 0) // aminos == iota((depth, depth), 1) // aminos)
    amino_d = iota((depth, LANES), 0) % aminos
    block = iota((pair_rows, LANES), 1) // PROJ_FEATURES
    for copy in left_copies:
        copy.wait_recv()
    left_all = side_buf[:, :tile].reshape(depth, LANES)
    right_all = dot(rep, side_buf[:, tile:].reshape(depth, LANES))
    right_all = jnp.concatenate(
        [jnp.where(amino_d == a, right_all, 0.0).astype(BF16) for a in range(aminos)], axis=1)
    product = dot(left_all, right_all, 0, 0)
    for a in range(aminos):
        product_buf[a * LANES:(a + 1) * LANES, :] = product[:, a * LANES:(a + 1) * LANES]
    for c in range(0, PROJ_FEATURES, aminos):
        slabs = [product_buf[pl.ds(c + x, pair_rows, stride=PROJ_FEATURES), :]
                 for x in range(aminos)]
        for j in range(aminos):
            turned = jnp.zeros((pair_rows, LANES), F32)
            for x in range(aminos):
                shift = (x - j) % aminos * PROJ_FEATURES
                moved = pltpu.roll(slabs[x], shift, 1) if shift else slabs[x]
                turned = jnp.where(block == x, moved, turned)
            lhs_buf[j * pair_rows:(j + 1) * pair_rows,
                    c * PROJ_FEATURES:c * PROJ_FEATURES + LANES] = turned.astype(BF16)
    loads[2].wait()
    outer = dot(lhs_buf[...], outer_ref[...])
    result = (pair_turned + pair_mask * (outer / counts)).astype(BF16)
    pair_out_ref[...] = dot(order, result, 0, 0).astype(BF16)

    for copy in out_copies:
        copy.wait_recv()
    out_ref[...] = out_buf[...]
    for copy in emb_copies + aux_copies + left_copies + out_copies:
        copy.wait_send()


def fused(*args):
    emb, mask, resolved, pair = args[:4]
    groups, ranks = lax.axis_size("seq"), lax.axis_size("res")
    chains, aminos = emb.shape[:2]
    tile = chains // ranks * aminos
    pair_rows = pair.shape[0]
    devices = groups * ranks
    vmem = pl.BlockSpec(memory_space=pltpu.VMEM)
    whole = pl.BlockSpec(memory_space=pl.ANY)
    dma = pltpu.SemaphoreType.DMA
    out, pair_out = pl.pallas_call(
        functools.partial(fused_kernel, groups, ranks, chains, aminos),
        out_shape=(
            jax.ShapeDtypeStruct(emb.shape, BF16),
            jax.ShapeDtypeStruct((pair_rows * aminos, CZ), BF16),
        ),
        in_specs=[vmem] * 4 + [whole, vmem, whole, vmem, whole],
        out_specs=(vmem, vmem),
        scratch_shapes=[
            pltpu.VMEM(emb.shape, BF16),
            pltpu.VMEM((devices, 2 * HEAD_NUMBER, LANES), BF16),
            pltpu.VMEM((devices, 2 * tile, LANES), BF16),
            pltpu.VMEM((devices, 2 * tile, LANES), BF16),
            pltpu.VMEM(emb.shape, BF16),
            pltpu.VMEM(emb.shape, BF16),
            pltpu.VMEM((pair_rows * PROJ_FEATURES, LANES), F32),
            pltpu.VMEM((pair_rows * aminos, PROJ_FEATURES * PROJ_FEATURES), BF16),
            pltpu.VMEM(args[4].shape, BF16),
            pltpu.VMEM(args[6].shape, BF16),
            pltpu.VMEM(args[8].shape, BF16),
            dma((ranks,)), dma((ranks,)), dma((devices,)), dma((devices,)),
            dma((devices,)), dma((devices,)), dma((ranks,)), dma((ranks,)), dma((3,)),
        ],
        compiler_params=pltpu.CompilerParams(collective_id=0, has_side_effects=True),
    )(
        emb, mask.T, resolved.reshape(1, -1),
        pair.reshape(-1, CZ), args[4], args[5].T, args[6], args[7].T, args[8],
    )
    return out, pair_out.reshape(pair.shape)


def fits(mesh, emb, pair):
    groups, ranks = mesh.shape["seq"], mesh.shape["res"]
    chains, aminos = emb.shape[:2]
    if chains % ranks or aminos * PROJ_FEATURES != LANES or chains * aminos != LANES:
        return False
    pairs = pair.shape[0] * aminos
    return pairs * groups == LANES and chains // ranks * aminos * groups == PROJ_FEATURES


def solution(mesh):
    placed = (
        P(("crop", "seq"), "res", None),
        P(("crop", "seq"), "res"),
        P("crop"),
        P(("crop", "seq"), "res", None),
        P(),
        P(),
        P(),
        P(),
        P(),
    )
    def either(*args):
        return (fused if fits(mesh, args[0], args[3]) else per_device)(*args)

    return jax.shard_map(
        either,
        mesh=mesh,
        in_specs=placed,
        out_specs=(P(("crop", "seq"), "res", None), P(("crop", "seq"), "res", None)),
        check_vma=False,
    )
```
